256 devices in a mesh: dp: 16 (over z_hi, y), outer: 16 (over z_lo, x, core).
Axes of the slice: x: 4, y: 4, z: 8 (z_hi: 4, z_lo: 2; z = z_hi * 2 + z_lo), core: 2. Of those that a mesh axis runs over, the one named last changes fastest.
Arguments:
- targets: bfloat16 [1024, 256], P(('dp', 'outer')), may hold values from -6 to 6
- behaviors: bfloat16 [1024, 1536, 256], P(('dp', 'outer')), may hold values from -256 to 256
- topk_index: int32 [1024, 1024], P(('dp', 'outer')), may hold values from 0 to 1535, as said below
- target_ids: int32 [1024], P(('dp', 'outer')), may hold values from 0 to 1073741823
- behavior_ids: int32 [1024, 1536], P(('dp', 'outer')), may hold values from 0 to 1073741823, as said below
- target_codes: int32 [1024], P(('dp', 'outer')), may hold values from 0 to 1073741823
- behavior_codes: int32 [1024, 1536], P(('dp', 'outer')), may hold values from 0 to 1073741823
- labels: int32 [1024], P(('dp', 'outer')), may hold values from -1 to 1, as said below
- attn_weights: float32 [4, 256, 256], replicated, may hold values from -2 to 2
- dense_weights: float32 [512, 1024], replicated, may hold values from -0.25 to 0.25
- head_weights: float32 [2, 1024], replicated, may hold values from -0.6 to 0.6
- moments: float32 [2, 788480], P(None, ('dp', 'outer')), may hold values from -0.0018 to 0.0018, as said below
Outputs:
- new_attention: float32 [4, 256, 256], replicated
- new_dense: float32 [512, 1024], replicated
- new_head: float32 [2, 1024], replicated
- new_moments: float32 [2, 788480], P(None, ('dp', 'outer'))
- loss: float32 [], replicated
The draws below stay inside these ranges and needn't reach their ends.
Inputs may be any that keep to these rules, and one draw needn't show every extreme that they name: `topk_index`: indices into a user's 1536 behaviors, distinct within a user. `behavior_ids`: item ids; a behavior may carry its own user's target id. `labels`: -1 marks a user without a label; user 1024 - 1 always has one. `moments`: row 1 is positive.
All inputs are finite; a program needn't handle non-finite values.
Results may differ from the reference program's by a relative error of at most 0.012.
The reference program's roundings to bfloat16 on the way (of `picked`, `queries`, `attend`, `attended`, `mixed_out` and `hidden`) count: a program that leaves them out, or rounds other values in their place, can miss the bound.
Values sent between devices are 32-bit elements; how exact they have to be, the bound alone decides.
No kernel may reach another device: no remote copies, remote signals or barrier semaphores. Data moves between devices by JAX's collectives and lax.ppermute only.
A program may use at most 64 MiB of HBM per device.

```python
import math
import jax
import jax.numpy as jnp
from jax import lax

D = 256
HEADS = 8
FF = 1024
K = 1024
HIST = 1536
B_DEV = 4
DH = 32
B = 1024
P_SIZE = 788480


def target_rows(key):
    return jnp.clip(jax.random.normal(jax.random.fold_in(key, 11), (B, D), jnp.float32), -6.0, 6.0)


def chosen_positions(key):
    key_list = jax.random.split(jax.random.fold_in(key, 12), B)
    return jax.vmap(lambda member: jax.random.permutation(member, HIST)[:K])(key_list).astype(jnp.int32)


def target_items(key):
    return jax.random.randint(jax.random.fold_in(key, 13), (B,), 0, 1073741824, jnp.int32)


def draw_targets(key, part):
    return target_rows(key).astype(jnp.bfloat16)


def draw_topk_index(key, part):
    return chosen_positions(key)


def draw_target_ids(key, part):
    return target_items(key)


def draw_behavior_ids(key, part):
    others = jax.random.randint(jax.random.fold_in(key, 14), (B, HIST), 0, 1073741824, jnp.int32)
    repeat = jax.random.randint(jax.random.fold_in(key, 15), (B, HIST), 0, 8, jnp.int32) == 0
    return jnp.where(repeat, target_items(key)[:, None], others).astype(jnp.int32)


def draw_labels(key, part):
    user_index = jnp.arange(B, dtype=jnp.int32)
    ticket = jax.random.randint(jax.random.fold_in(key, 21), (B,), 0, 4 * (B - 1), jnp.int32)
    labeled = (ticket < B - 1 + 2 * user_index) | (user_index == B - 1)
    clicks = (jax.random.randint(jax.random.fold_in(key, 22), (B,), 0, 20, jnp.int32) < 7).astype(jnp.int32)
    return jnp.where(labeled, clicks, -1).astype(jnp.int32)


def draw_behaviors(key, part):
    drawn_rows = jnp.clip(jax.random.normal(jax.random.fold_in(key, 16), (B, HIST, D), jnp.float32), -6.0, 6.0)
    return drawn_rows.astype(jnp.bfloat16)


def draw_attn_weights(key, part):
    drawn_rows = jnp.clip(jax.random.normal(jax.random.fold_in(key, 20), (4, D, D), jnp.float32), -6.0, 6.0) * D ** (-0.5)
    return drawn_rows


def draw_moments(key, part):
    first_row = jnp.clip(jax.random.normal(jax.random.fold_in(key, 23), (P_SIZE,), jnp.float32) * 0.0003, -0.0018, 0.0018)
    second_row = jnp.exp(jax.random.uniform(jax.random.fold_in(key, 24), (P_SIZE,), jnp.float32, math.log(1e-08), math.log(1e-06)))
    return jnp.stack([first_row, second_row])


def place_ends(result, stream_key, least, top_value):
    spot = [jax.random.randint(jax.random.fold_in(stream_key, axis), (), 0, length) for axis, length in enumerate(result.shape)]
    main_axis = result.shape.index(max(result.shape))
    next_to = spot[:main_axis] + [(spot[main_axis] + 1) % result.shape[main_axis]] + spot[main_axis + 1:]
    return result.at[tuple(spot)].set(least).at[tuple(next_to)].set(top_value)


def normal_values(key, dims, deviation, most, held_as=jnp.bfloat16):
    entries = jax.random.normal(key, dims, jnp.float32) * deviation
    return jnp.minimum(jnp.maximum(entries, -most), most).astype(held_as)


def setup_inputs(seed: int = 0) -> dict:
    key_of = jax.random.split(jax.random.key(seed), 13)
    targets = draw_targets(jax.random.fold_in(key_of[12], 71), 0)
    behaviors = draw_behaviors(jax.random.fold_in(key_of[12], 71), 0)
    topk_index = draw_topk_index(jax.random.fold_in(key_of[12], 71), 0)
    target_ids = draw_target_ids(jax.random.fold_in(key_of[12], 71), 0)
    behavior_ids = draw_behavior_ids(jax.random.fold_in(key_of[12], 71), 0)
    target_codes = place_ends(jax.random.randint(key_of[5], (B,), 0, 1073741824), jax.random.fold_in(key_of[5], 1), 0, 1073741823).astype(jnp.int32)
    behavior_codes = place_ends(jax.random.randint(key_of[6], (B, HIST), 0, 1073741824), jax.random.fold_in(key_of[6], 1), 0, 1073741823).astype(jnp.int32)
    labels = draw_labels(jax.random.fold_in(key_of[12], 71), 0)
    attn_weights = draw_attn_weights(jax.random.fold_in(key_of[12], 71), 0)
    dense_weights = normal_values(key_of[9], (2 * D, FF), (2 * D) ** -0.5, 0.25, jnp.float32)
    head_weights = normal_values(key_of[10], (2, FF), 0.1, 0.6, jnp.float32)
    moments = draw_moments(jax.random.fold_in(key_of[12], 71), 0)
    return dict(targets=targets, behaviors=behaviors, topk_index=topk_index, target_ids=target_ids, behavior_ids=behavior_ids, target_codes=target_codes, behavior_codes=behavior_codes, labels=labels, attn_weights=attn_weights, dense_weights=dense_weights, head_weights=head_weights, moments=moments)


sim_weight = 4.0
masked_score = -1000000000.0
learn_rate = 0.001
first_decay = 0.9
second_decay = 0.99
adam_eps = 1e-08
first_fix = 1.0 - 0.9 ** 20
second_fix = 1.0 - 0.99 ** 20

def count_bits(value):
    value = value.astype(jnp.int32)
    value = value - jnp.bitwise_and(jnp.right_shift(value, 1), jnp.int32(1431655765))
    value = jnp.bitwise_and(value, jnp.int32(858993459)) + jnp.bitwise_and(jnp.right_shift(value, 2), jnp.int32(858993459))
    value = jnp.bitwise_and(value + jnp.right_shift(value, 4), jnp.int32(252645135))
    value = value + jnp.right_shift(value, 8)
    value = value + jnp.right_shift(value, 16)
    return jnp.bitwise_and(value, jnp.int32(63)).astype(jnp.int32)

def block_loss(weights, targets, picked, similarity, excluded, labels):
    attention, dense, head_rows = weights
    attention_half = attention.astype(jnp.bfloat16)
    dense_half = dense.astype(jnp.bfloat16)
    user_count = picked.shape[0]
    pick_count = picked.shape[1]
    queries = jnp.dot(targets, attention_half[0], preferred_element_type=jnp.float32).astype(jnp.bfloat16)
    flat_rows = picked.reshape(user_count * pick_count, D)
    key_rows = jnp.dot(flat_rows, attention_half[1], preferred_element_type=jnp.float32).astype(jnp.bfloat16)
    value_rows = jnp.dot(flat_rows, attention_half[2], preferred_element_type=jnp.float32).astype(jnp.bfloat16)
    key_rows = key_rows.reshape(user_count, pick_count, HEADS, DH)
    value_rows = value_rows.reshape(user_count, pick_count, HEADS, DH)
    head_queries = queries.reshape(user_count, HEADS, DH)
    scores = jnp.einsum('uhd,ukhd->uhk', head_queries.astype(jnp.float32), key_rows.astype(jnp.float32)) * DH ** (-0.5)
    scores = scores + similarity[:, None, :]
    scores = jnp.where(excluded[:, None, :], masked_score, scores)
    attend = jax.nn.softmax(scores, axis=-1).astype(jnp.bfloat16)
    attended = jnp.einsum('uhk,ukhd->uhd', attend.astype(jnp.float32), value_rows.astype(jnp.float32))
    attended = attended.astype(jnp.bfloat16).reshape(user_count, D)
    mixed_out = jnp.dot(attended, attention_half[3], preferred_element_type=jnp.float32).astype(jnp.bfloat16)
    inputs = jnp.concatenate([targets, mixed_out], axis=1)
    pre_act = jnp.dot(inputs, dense_half, preferred_element_type=jnp.float32) + head_rows[0]
    hidden = jax.nn.gelu(pre_act, approximate=False).astype(jnp.bfloat16)
    logits = jnp.dot(hidden, head_rows[1].astype(jnp.bfloat16), preferred_element_type=jnp.float32)
    labeled = labels >= 0
    target_click = jnp.where(labeled, labels, 0).astype(jnp.float32)
    per_user = jax.nn.softplus(logits) - target_click * logits
    return jnp.sum(jnp.where(labeled, per_user, 0.0))

def reference(targets, behaviors, topk_index, target_ids, behavior_ids, target_codes, behavior_codes, labels, attn_weights, dense_weights, head_weights, moments):
    label_total = jnp.sum((labels >= 0).astype(jnp.float32))
    block_count = B // B_DEV
    weights = (attn_weights, dense_weights, head_weights)

    def split_rows(array):
        return array.reshape((block_count, B_DEV) + array.shape[1:])

    def advance(carry, block):
        totals, loss_sum = carry
        block_targets, block_rows, block_index, block_ids, block_behavior_ids, block_codes, block_behavior_codes, block_labels = block
        picked = jnp.take_along_axis(block_rows, block_index[:, :, None], axis=1)
        picked_ids = jnp.take_along_axis(block_behavior_ids, block_index, axis=1)
        picked_codes = jnp.take_along_axis(block_behavior_codes, block_index, axis=1)
        excluded = picked_ids == block_ids[:, None]
        agreement = 15 - count_bits(jnp.bitwise_xor(picked_codes, block_codes[:, None]))
        similarity = sim_weight * agreement.astype(jnp.float32) / 15.0

        def objective(params):
            return block_loss(params, block_targets, picked, similarity, excluded, block_labels) / label_total
        local_sum, pullback = jax.vjp(objective, weights)
        gradients = pullback(jnp.ones_like(local_sum))[0]
        totals = jax.tree.map(jnp.add, totals, gradients)
        return ((totals, loss_sum + local_sum), None)
    start = (jax.tree.map(jnp.zeros_like, weights), jnp.zeros((), jnp.float32))
    blocks = (split_rows(targets), split_rows(behaviors), split_rows(topk_index), split_rows(target_ids), split_rows(behavior_ids), split_rows(target_codes), split_rows(behavior_codes), split_rows(labels))
    (gradients, loss), unused = lax.scan(advance, start, blocks)
    flat_grads = jnp.concatenate([portion.reshape(-1) for portion in gradients])
    flat_weights = jnp.concatenate([portion.reshape(-1) for portion in weights])
    new_first = first_decay * moments[0] + (1.0 - first_decay) * flat_grads
    new_second = second_decay * moments[1] + (1.0 - second_decay) * flat_grads * flat_grads
    new_flat = flat_weights - learn_rate * (new_first / first_fix) / (jnp.sqrt(new_second / second_fix) + adam_eps)
    attn_size = attn_weights.size
    dense_size = dense_weights.size
    new_attention = new_flat[:attn_size].reshape(attn_weights.shape)
    new_dense = new_flat[attn_size:attn_size + dense_size].reshape(dense_weights.shape)
    new_head = new_flat[attn_size + dense_size:].reshape(head_weights.shape)
    return (new_attention, new_dense, new_head, jnp.stack([new_first, new_second]), loss)
```

```python
import jax
import jax.numpy as jnp
from jax import lax
from jax.experimental import pallas as pl
from jax.experimental.pallas import tpu as pltpu
from jax.sharding import Mesh
from jax.sharding import PartitionSpec as P

D = 256
HEADS = 8
DH = 32
FF = 1024
K = 1024
HIST = 1536
U = 4
LANES = 128
ROWS = 6160
SHARE = 3080
BLOCK = 385
MAIN = 24
CHUNK = 200
AXES = ("zh", "y", "zl", "x", "c")
SIZES = dict(zh=4, y=4, zl=2, x=4, c=2)

sim_weight = 4.0
masked_score = -1000000000.0
unpicked_score = -3e38
learn_rate = 0.001
first_decay = 0.9
second_decay = 0.99
adam_eps = 1e-08
first_fix = 1.0 - 0.9**20
second_fix = 1.0 - 0.99**20

f32 = jnp.float32
bf16 = jnp.bfloat16


def iota(shape, dim):
    return lax.broadcasted_iota(jnp.int32, shape, dim)


def dot(a, b, contract):
    return lax.dot_general(a, b, ((contract[:1], contract[1:]), ((), ())), preferred_element_type=f32)


def halves(x):
    high = x.astype(bf16)
    return jnp.concatenate([high, (x - high.astype(f32)).astype(bf16)], axis=0)


def both(x):
    n = x.shape[0] // 2
    return x[:n] + x[n:]


def count_bits(value):
    value = value - ((value >> 1) & 1431655765)
    value = (value & 858993459) + ((value >> 2) & 858993459)
    value = (value + (value >> 4)) & 252645135
    value = value + (value >> 8)
    value = value + (value >> 16)
    return value & 63


def window_rows(zh, y, zl, x, c):
    return BLOCK * (4 * zh + y) + MAIN * (8 * zl + 2 * x + c)


def windows(half):
    for i in range(4):
        for j in range(4):
            x, y = (i, j) if half == 0 else (j, i)
            for z in range(8):
                base = CHUNK * (4 * i + j)
                place = (z // 2, y, z % 2, x, half)
                yield base + MAIN * z, base + 8 * MAIN + z, window_rows(*place), place


def column(ref):
    at = iota((U, 1), 0)
    out = jnp.full((U, 1), ref[0], ref.dtype)
    for u in range(1, U):
        out = jnp.where(at == u, ref[u], out)
    return out


def grad_body(
    target_ids,
    target_codes,
    labels,
    targets,
    topk_index,
    behavior_ids,
    behavior_codes,
    behaviors_hbm,
    attn_hbm,
    dense_hbm,
    head,
    keep,
    send,
    rows,
    attn,
    dense,
    behaviors,
    sems,
):
    copies = [pltpu.make_async_copy(attn_hbm.at[i], attn.at[i], sems.at[i]) for i in range(4)]
    copies += [pltpu.make_async_copy(behaviors_hbm.at[u], behaviors.at[u], sems.at[4 + u]) for u in range(U)]
    copies += [pltpu.make_async_copy(dense_hbm, dense, sems.at[8])]
    order = [0, 1, 4, 5, 6, 7, 2, 3, 8]
    for i in order:
        copies[i].start()

    picked = []
    for u in range(U):
        index = topk_index[u : u + 1, :]
        coarse = jnp.where(iota((16, K), 0) == (index >> 7), 1.0, 0.0).astype(bf16)
        fine = jnp.where(iota((LANES, K), 0) == (index & 127), 1.0, 0.0).astype(bf16)
        table = dot(coarse, fine, (1, 1))
        picked.append(
            jnp.concatenate(
                [jnp.broadcast_to(table[k : k + 1, :], (HEADS, LANES)) for k in range(HIST // LANES)], axis=1
            )
        )
    agreement = 15 - count_bits(behavior_codes[...] ^ column(target_codes))
    similarity = sim_weight * agreement.astype(f32) / 15.0
    excluded = jnp.where(behavior_ids[...] == column(target_ids), 1.0, 0.0)

    def per_head(x):
        return jnp.concatenate([jnp.broadcast_to(x[u : u + 1, :], (HEADS, x.shape[1])) for u in range(U)], axis=0)

    similarity = per_head(similarity)
    excluded = per_head(excluded) > 0.5
    picked = jnp.concatenate(picked, axis=0) > 0.5
    head_mask = (iota((U * HEADS, D), 1) // DH) == (iota((U * HEADS, D), 0) % HEADS)

    def spread(x):
        return jnp.where(head_mask, per_head(x), 0.0)

    def fold(x):
        kept = jnp.where(head_mask, x, 0.0)
        return jnp.concatenate(
            [jnp.sum(kept[HEADS * u : HEADS * (u + 1)], axis=0, keepdims=True) for u in range(U)], axis=0
        )

    def rows_by_user(x, contract):
        out = []
        for u in range(U):
            out.append(both(dot(halves(x[HEADS * u : HEADS * (u + 1)]), behaviors[u], contract)))
        return jnp.concatenate(out, axis=0)

    goals = targets[...]
    copies[0].wait()
    queries = dot(goals, attn[0].astype(bf16), (1, 0)).astype(bf16).astype(f32)
    query_blocks = spread(queries)
    copies[1].wait()
    w_key = attn[1].astype(bf16)
    query_fold = dot(query_blocks.astype(bf16), w_key, (1, 1))
    for u in range(U):
        copies[4 + u].wait()
    scores = rows_by_user(query_fold, (1, 1)) * DH ** (-0.5) + similarity
    scores = jnp.where(excluded, masked_score, scores)
    scores = jnp.where(picked, scores, unpicked_score)
    top = jnp.max(scores, axis=1, keepdims=True)
    weight = jnp.exp(scores - top)
    weight = weight / jnp.sum(weight, axis=1, keepdims=True)
    attend = weight.astype(bf16)
    mean_rows = jnp.concatenate(
        [dot(attend[HEADS * u : HEADS * (u + 1)], behaviors[u], (1, 0)) for u in range(U)], axis=0
    )
    copies[2].wait()
    w_value = attn[2].astype(bf16)
    attended = fold(both(dot(halves(mean_rows), w_value, (1, 0)))).astype(bf16)
    copies[3].wait()
    w_out = attn[3].astype(bf16)
    mixed = dot(attended, w_out, (1, 0)).astype(bf16)
    copies[8].wait()
    w_top = dense[:D].astype(bf16)
    w_low = dense[D:].astype(bf16)
    pre = dot(goals, w_top, (1, 0)) + dot(mixed, w_low, (1, 0)) + head[0:1, :]
    inner = 0.5 * (1.0 + lax.erf(pre * 0.5**0.5))
    hidden = (pre * inner).astype(bf16).astype(f32)
    head_vector = head[1:2, :].astype(bf16).astype(f32)
    logits = jnp.sum(hidden * head_vector, axis=1, keepdims=True)
    marks = column(labels)
    labeled = marks >= 0
    click = jnp.where(labeled, marks, 0).astype(f32)
    small = jnp.exp(-jnp.abs(logits))
    soft = jnp.maximum(logits, 0.0) + jnp.log1p(small)
    loss = jnp.sum(jnp.where(labeled, soft - click * logits, 0.0), axis=0, keepdims=True)
    count = jnp.sum(jnp.where(labeled, 1.0, 0.0), axis=0, keepdims=True)

    chance = jnp.where(logits >= 0, 1.0, small) / (1.0 + small)
    d_logits = jnp.where(labeled, chance - click, 0.0)
    d_hidden = (d_logits * head_vector).astype(bf16).astype(f32)
    d_pre = d_hidden * (inner + pre * jnp.exp(-0.5 * pre * pre) * (2.0 * jnp.pi) ** -0.5)
    d_pre_halves = halves(d_pre)
    d_mixed = both(dot(d_pre_halves, w_low, (1, 1))).astype(bf16)
    d_attended = dot(d_mixed, w_out, (1, 1)).astype(bf16)
    d_blocks = spread(d_attended.astype(f32))
    value_fold = dot(d_blocks.astype(bf16), w_value, (1, 1))
    d_attend = rows_by_user(value_fold, (1, 1)).astype(bf16).astype(f32)
    d_scores = weight * (d_attend - jnp.sum(weight * d_attend, axis=1, keepdims=True))
    d_scores = jnp.where(excluded, 0.0, d_scores)
    score_rows = rows_by_user(d_scores, (1, 0)) * DH ** (-0.5)
    d_queries = fold(both(dot(halves(score_rows), w_key, (1, 0)))).astype(bf16)

    def outer(a, b):
        return dot(a, b, (0, 0))

    def twice(x):
        return jnp.concatenate([x, x], axis=0)

    grads = [
        outer(goals, d_queries),
        outer(halves(score_rows), twice(query_blocks.astype(bf16))),
        outer(halves(mean_rows), twice(d_blocks.astype(bf16))),
        outer(attended, d_mixed),
    ]
    for i in range(4):
        for part in range(2):
            rows[pl.ds(512 * i + part, D, stride=2), :] = grads[i][:, LANES * part : LANES * (part + 1)]
    for source in range(2):
        grad = outer(twice((goals, mixed)[source]), d_pre_halves)
        for part in range(8):
            rows[pl.ds(2048 + 2048 * source + part, D, stride=8), :] = grad[:, LANES * part : LANES * (part + 1)]
    d_bias = jnp.sum(d_pre, axis=0, keepdims=True)
    d_vector = jnp.sum(d_logits * hidden, axis=0, keepdims=True)
    for source in range(2):
        grad = (d_bias, d_vector)[source]
        for part in range(8):
            at = 6144 + 8 * source + part
            rows[at : at + 1, :] = grad[:, LANES * part : LANES * (part + 1)]

    lane = iota((8, LANES), 1)
    first = (iota((8, LANES), 0) == 0) & (lane < 2)
    front = jnp.where(lane == 0, loss, count)
    lane = iota((1, LANES), 1)
    back = jnp.where(lane == LANES - 2, loss, count)

    def place(half, out):
        for main, tail, start, where in windows(half):
            for k in range(0, MAIN, 8):
                piece = rows[start + k : start + k + 8, :]
                if where[2] == 1 and k == 0:
                    piece = jnp.where(first, front, piece)
                out[main + k : main + k + 8, :] = piece
            last = rows[start + MAIN : start + MAIN + 1, :]
            if where[2] == 0:
                last = jnp.where(lane >= LANES - 2, back, last)
            out[tail : tail + 1, :] = last

    core = lax.axis_index("c")

    @pl.when(core == 0)
    def _():
        place(0, keep)
        place(1, send)

    @pl.when(core == 1)
    def _():
        place(1, keep)
        place(0, send)


VMEM = pl.BlockSpec(memory_space=pltpu.VMEM)
SMEM = pl.BlockSpec(memory_space=pltpu.SMEM)
ANY = pl.BlockSpec(memory_space=pl.ANY)
PARAMS = pltpu.CompilerParams(vmem_limit_bytes=50 * 2**20)


def vmem(*shape):
    return jax.ShapeDtypeStruct(shape, f32)


def call(body, outs, *args, specs=None, out_specs=None, scratch=()):
    return pl.pallas_call(
        body,
        out_shape=outs,
        in_specs=specs or [VMEM] * len(args),
        out_specs=out_specs or jax.tree.map(lambda _: VMEM, outs),
        scratch_shapes=scratch,
        compiler_params=PARAMS,
    )(*args)


def position(stage):
    x, y, c = (lax.axis_index(a) for a in ("x", "y", "c"))
    return jnp.where((c == 0) == (stage == 0), x, y)


def split_body(stage, parts):
    def body(*refs):
        sources, outs = refs[:parts], refs[parts:]
        size = outs[0].shape[0]
        at = position(stage)
        for k in range(4):
            start = pl.multiple_of(((at + k) % 4) * size, 8)
            total = sources[0][pl.ds(start, size), :]
            for s in sources[1:]:
                total = total + s[pl.ds(start, size), :]
            outs[k][...] = total

    return body


def z_split_body(*refs):
    sources, out = refs[:4], refs[4]
    total = sources[0][...] + sources[1][...] + sources[2][...] + sources[3][...]
    for z in range(8):
        out[z, :MAIN, :] = total[MAIN * z : MAIN * (z + 1)]
        tail = total[8 * MAIN + z : 8 * MAIN + z + 1]
        out[z, MAIN:, :] = jnp.where(iota((8, LANES), 0) == 0, tail, 0.0)


def adam_body(parts, moments, spread, new_moments, loss_out):
    total = parts[0]
    for z in range(1, 8):
        total = total + parts[z]
    zl, x, c = (lax.axis_index(a) for a in ("zl", "x", "c"))
    shift = 8 * (8 * zl + 2 * x + c)
    tail = total[MAIN : MAIN + 1]
    line = jnp.where(zl == 0, tail, total[0:1])
    lane = iota((1, LANES), 1)
    loss_at = jnp.where(zl == 0, LANES - 2, 0)
    loss = jnp.sum(jnp.where(lane == loss_at, line, 0.0), axis=1, keepdims=True)
    count = jnp.sum(jnp.where(lane == loss_at + 1, line, 0.0), axis=1, keepdims=True)
    loss_out[...] = loss / count
    lanes = iota((32, LANES), 1)
    turned = pltpu.roll(total, (LANES - shift) % LANES, 1)
    after = pltpu.roll(turned, 31, 0)
    grads = jnp.where(lanes < LANES - shift, turned, after) / count
    old = []
    for k in range(24):
        old.append(moments[:, LANES * k : LANES * (k + 1)])
    last = moments[:, SHARE - LANES :]
    last = jnp.where(iota((2, LANES), 1) < SHARE - 24 * LANES, pltpu.roll(last, SHARE - 24 * LANES, 1), 1.0)
    old.append(last)
    one = jnp.ones((7, LANES), f32)
    first = jnp.concatenate([o[0:1] for o in old] + [one], axis=0)
    second = jnp.concatenate([o[1:2] for o in old] + [one], axis=0)
    new_first = first_decay * first + (1.0 - first_decay) * grads
    new_second = second_decay * second + (1.0 - second_decay) * grads * grads
    for k in range(25):
        wide = min(LANES, SHARE - LANES * k)
        new_moments[0:1, LANES * k : LANES * k + wide] = new_first[k : k + 1, :wide]
        new_moments[1:2, LANES * k : LANES * k + wide] = new_second[k : k + 1, :wide]
    step = learn_rate * (new_first / first_fix) / (jnp.sqrt(new_second / second_fix) + adam_eps)
    flat = iota((32, LANES), 0) * LANES + lanes
    step = jnp.where(flat < SHARE, step, 0.0)
    turned = pltpu.roll(step, shift, 1)
    before = pltpu.roll(turned, 1, 0)
    step = jnp.where(lanes >= shift, turned, before)
    for z in range(8):
        spread[z] = step


def z_join_body(parts, out):
    for z in range(8):
        out[MAIN * z : MAIN * (z + 1), :] = parts[z, :MAIN, :]
        out[8 * MAIN + z : 8 * MAIN + z + 1, :] = parts[z, MAIN : MAIN + 1, :]


def join_body(stage):
    def body(*refs):
        sources, out = refs[:4], refs[4]
        size = sources[0].shape[0]
        at = position(stage)
        for k in range(4):
            start = pl.multiple_of(((at + 4 - k) % 4) * size, 8)
            out[pl.ds(start, size), :] = sources[k][...]

    return body


def apply_body(mine, other, attn, dense, head, new_attn, new_dense, new_head, rows):
    def place(half, source):
        for main, tail, start, where in windows(half):
            rows[start + 1 : start + MAIN, :] = source[main + 1 : main + MAIN, :]

    def joints(even, odd):
        firsts, lasts = {}, {}
        for half, source in ((0, even), (1, odd)):
            for main, tail, start, where in windows(half):
                firsts[start] = (source, main)
                lasts[start + MAIN] = (source, tail)
        for at in sorted(firsts | lasts):
            total = [r[m : m + 1, :] for r, m in (d[at] for d in (firsts, lasts) if at in d)]
            rows[at : at + 1, :] = sum(total[1:], total[0])

    core = lax.axis_index("c")
    for c in range(2):

        @pl.when(core == c)
        def _():
            place(c, mine)
            place(1 - c, other)
            joints(*((mine, other) if c == 0 else (other, mine)))

    for i in range(4):
        for part in range(2):
            lanes = slice(LANES * part, LANES * (part + 1))
            new_attn[i, :, lanes] = attn[i, :, lanes] - rows[pl.ds(512 * i + part, D, stride=2), :]
    for part in range(8):
        lanes = slice(LANES * part, LANES * (part + 1))
        new_dense[:, lanes] = dense[:, lanes] - rows[pl.ds(2048 + part, 2 * D, stride=8), :]
    for source in range(2):
        for part in range(8):
            lanes = slice(LANES * part, LANES * (part + 1))
            at = 6144 + 8 * source + part
            new_head[source : source + 1, lanes] = head[source : source + 1, lanes] - rows[at : at + 1, :]


def places():
    for zh in range(4):
        for y in range(4):
            for zl in range(2):
                for x in range(4):
                    for c in range(2):
                        yield zh, y, zl, x, c


def number(zh, y, zl, x, c):
    return (((zh * 4 + y) * 2 + zl) * 4 + x) * 2 + c


def turn(stage, k):
    pairs = []
    for zh, y, zl, x, c in places():
        along_x = (c == 0) == (stage == 0)
        goal = (zh, y, zl, (x + k) % 4, c) if along_x else (zh, (y + k) % 4, zl, x, c)
        pairs.append((number(zh, y, zl, x, c), number(*goal)))
    return pairs


def swap(x):
    return lax.ppermute(x, "c", [(0, 1), (1, 0)])


def gradient_windows(targets, behaviors, topk_index, target_ids, behavior_ids, target_codes, behavior_codes, labels, attn_weights, dense_weights, head_weights):
    return call(
        grad_body,
        (vmem(3200, LANES), vmem(3200, LANES)),
        target_ids,
        target_codes,
        labels,
        targets,
        topk_index,
        behavior_ids,
        behavior_codes,
        behaviors,
        attn_weights,
        dense_weights,
        head_weights,
        specs=[SMEM] * 3 + [VMEM] * 4 + [ANY] * 3 + [VMEM],
        scratch=[
            pltpu.VMEM((ROWS, LANES), f32),
            pltpu.VMEM((4, D, D), f32),
            pltpu.VMEM((2 * D, FF), f32),
            pltpu.VMEM((U, HIST, D), bf16),
            pltpu.SemaphoreType.DMA((9,)),
        ],
    )


def per_device(
    targets,
    behaviors,
    topk_index,
    target_ids,
    behavior_ids,
    target_codes,
    behavior_codes,
    labels,
    attn_weights,
    dense_weights,
    head_weights,
    moments,
):
    keep, send = gradient_windows(
        targets, behaviors, topk_index, target_ids, behavior_ids, target_codes, behavior_codes, labels, attn_weights, dense_weights, head_weights
    )
    own, *sent = call(split_body(0, 2), (vmem(800, LANES),) * 4, keep, swap(send))
    got = [lax.ppermute(s, AXES, turn(0, k + 1)) for k, s in enumerate(sent)]
    own, *sent = call(split_body(1, 4), (vmem(CHUNK, LANES),) * 4, own, *got)
    got = [lax.ppermute(s, AXES, turn(1, k + 1)) for k, s in enumerate(sent)]
    parts = call(z_split_body, vmem(8, 32, LANES), own, *got)
    parts = lax.all_to_all(parts, ("zh", "zl"), 0, 0, tiled=True)
    parts, new_moments, loss = call(
        adam_body, (vmem(8, 32, LANES), vmem(2, SHARE), vmem(1, 1)), parts, moments
    )
    parts = lax.all_to_all(parts, ("zh", "zl"), 0, 0, tiled=True)
    own = call(z_join_body, vmem(CHUNK, LANES), parts)
    got = [lax.ppermute(own, AXES, turn(1, k)) for k in range(1, 4)]
    own = call(join_body(1), vmem(800, LANES), own, *got)
    got = [lax.ppermute(own, AXES, turn(0, k)) for k in range(1, 4)]
    own = call(join_body(0), vmem(3200, LANES), own, *got)
    new_attention, new_dense, new_head = call(
        apply_body,
        (vmem(4, D, D), vmem(2 * D, FF), vmem(2, FF)),
        own,
        swap(own),
        attn_weights,
        dense_weights,
        head_weights,
        scratch=[pltpu.VMEM((ROWS, LANES), f32)],
    )
    return (new_attention, new_dense, new_head, new_moments, loss[0, 0])


def solution(mesh):
    finer = Mesh(mesh.devices.reshape(4, 4, 2, 4, 2), AXES)
    placed = (
        P(AXES, None),
        P(AXES, None, None),
        P(AXES, None),
        P(AXES),
        P(AXES, None),
        P(AXES),
        P(AXES, None),
        P(AXES),
        P(),
        P(),
        P(),
        P(None, AXES),
    )
    return jax.shard_map(
        per_device,
        mesh=finer,
        in_specs=placed,
        out_specs=(P(), P(), P(), P(None, AXES), P()),
        check_vma=False,
    )
```

```python
import jax
import jax.numpy as jnp
from jax import lax
from jax.experimental import pallas as pl
from jax.experimental.pallas import tpu as pltpu
from jax.sharding import Mesh
from jax.sharding import PartitionSpec as P

D = 256
HEADS = 8
DH = 32
FF = 1024
K = 1024
HIST = 1536
U = 4
LANES = 128
ROWS = 6160
SHARE = 3080
BLOCK = 385
MAIN = 24
UNIT = 104
STREAM = 16 * UNIT
AXES = ("zh", "y", "zl", "x", "c")
SIZES = dict(zh=4, y=4, zl=2, x=4, c=2)

sim_weight = 4.0
masked_score = -1000000000.0
unpicked_score = -3e38
learn_rate = 0.001
first_decay = 0.9
second_decay = 0.99
adam_eps = 1e-08
first_fix = 1.0 - 0.9**20
second_fix = 1.0 - 0.99**20

f32 = jnp.float32
bf16 = jnp.bfloat16


def iota(shape, dim):
    return lax.broadcasted_iota(jnp.int32, shape, dim)


def dot(a, b, contract):
    return lax.dot_general(a, b, ((contract[:1], contract[1:]), ((), ())), preferred_element_type=f32)


def halves(x):
    high = x.astype(bf16)
    return jnp.concatenate([high, (x - high.astype(f32)).astype(bf16)], axis=0)


def both(x):
    n = x.shape[0] // 2
    return x[:n] + x[n:]


def count_bits(value):
    value = value - ((value >> 1) & 1431655765)
    value = (value & 858993459) + ((value >> 2) & 858993459)
    value = (value + (value >> 4)) & 252645135
    value = value + (value >> 8)
    value = value + (value >> 16)
    return value & 63


def window_rows(zh, y, zl, x, c):
    return BLOCK * (4 * zh + y) + MAIN * (8 * zl + 2 * x + c)


def along(stream, step):
    return (stream + step) % 4


def bit_of(bit, x, y):
    v = x if bit < 2 else y
    q = (v >> 1) & 1
    return q if bit % 2 else (v & 1) ^ q


def unbits(bits):
    return bits[0] ^ (3 * bits[1]), bits[2] ^ (3 * bits[3])


def windows(half):
    for part in range(2):
        stream = 2 * half + part
        for at in range(16):
            bits = [0] * 4
            for step in range(4):
                bits[along(stream, step)] = (at >> (3 - step)) & 1
            x, y = unbits(bits)
            base = STREAM * part + UNIT * at
            for k in range(4):
                z = 4 * part + k
                place = (z // 2, y, z % 2, x, half)
                yield base + MAIN * k, base + 4 * MAIN + k, window_rows(*place), place


def column(ref):
    at = iota((U, 1), 0)
    out = jnp.full((U, 1), ref[0], ref.dtype)
    for u in range(1, U):
        out = jnp.where(at == u, ref[u], out)
    return out


def grad_body(
    *refs,
):
    sources, (keep, send, rows), targets_of, sems = refs[:11], refs[11:14], refs[14:25], refs[25]
    target_ids, target_codes, labels, targets, topk_index, behavior_ids, behavior_codes, head, behaviors, attn, dense = targets_of
    behaviors_hbm, attn_hbm, dense_hbm = sources[8:]
    little = [pltpu.make_async_copy(a, b, sems.at[9 + i]) for i, (a, b) in enumerate(zip(sources[:8], targets_of[:8]))]
    for i in (4, 0, 1, 2, 3, 5, 6, 7):
        little[i].start()
    copies = [pltpu.make_async_copy(attn_hbm.at[i], attn.at[i], sems.at[i]) for i in range(4)]
    copies += [pltpu.make_async_copy(behaviors_hbm.at[u], behaviors.at[u], sems.at[4 + u]) for u in range(U)]
    copies += [pltpu.make_async_copy(dense_hbm, dense, sems.at[8])]
    order = [0, 1, 4, 5, 6, 7, 2, 3, 8]
    for i in order:
        copies[i].start()

    for copy in little:
        copy.wait()

    picked = []
    for u in range(U):
        index = topk_index[u : u + 1, :]
        coarse = jnp.where(iota((16, K), 0) == (index >> 7), 1.0, 0.0).astype(bf16)
        fine = jnp.where(iota((LANES, K), 0) == (index & 127), 1.0, 0.0).astype(bf16)
        table = dot(coarse, fine, (1, 1))
        picked.append(
            jnp.concatenate(
                [jnp.broadcast_to(table[k : k + 1, :], (HEADS, LANES)) for k in range(HIST // LANES)], axis=1
            )
        )
    agreement = 15 - count_bits(behavior_codes[...] ^ column(target_codes))
    similarity = sim_weight * agreement.astype(f32) / 15.0
    excluded = jnp.where(behavior_ids[...] == column(target_ids), 1.0, 0.0)

    def per_head(x):
        return jnp.concatenate([jnp.broadcast_to(x[u : u + 1, :], (HEADS, x.shape[1])) for u in range(U)], axis=0)

    similarity = per_head(similarity)
    excluded = per_head(excluded) > 0.5
    picked = jnp.concatenate(picked, axis=0) > 0.5
    head_mask = (iota((U * HEADS, D), 1) // DH) == (iota((U * HEADS, D), 0) % HEADS)

    def spread(x):
        return jnp.where(head_mask, per_head(x), 0.0)

    def fold(x):
        kept = jnp.where(head_mask, x, 0.0)
        return jnp.concatenate(
            [jnp.sum(kept[HEADS * u : HEADS * (u + 1)], axis=0, keepdims=True) for u in range(U)], axis=0
        )

    def rows_by_user(x, contract):
        out = []
        for u in range(U):
            out.append(both(dot(halves(x[HEADS * u : HEADS * (u + 1)]), behaviors[u], contract)))
        return jnp.concatenate(out, axis=0)

    goals = targets[...]
    copies[0].wait()
    queries = dot(goals, attn[0].astype(bf16), (1, 0)).astype(bf16).astype(f32)
    query_blocks = spread(queries)
    copies[1].wait()
    w_key = attn[1].astype(bf16)
    query_fold = dot(query_blocks.astype(bf16), w_key, (1, 1))
    for u in range(U):
        copies[4 + u].wait()
    scores = rows_by_user(query_fold, (1, 1)) * DH ** (-0.5) + similarity
    scores = jnp.where(excluded, masked_score, scores)
    scores = jnp.where(picked, scores, unpicked_score)
    top = jnp.max(scores, axis=1, keepdims=True)
    weight = jnp.exp(scores - top)
    weight = weight / jnp.sum(weight, axis=1, keepdims=True)
    attend = weight.astype(bf16)
    mean_rows = jnp.concatenate(
        [dot(attend[HEADS * u : HEADS * (u + 1)], behaviors[u], (1, 0)) for u in range(U)], axis=0
    )
    copies[2].wait()
    w_value = attn[2].astype(bf16)
    attended = fold(both(dot(halves(mean_rows), w_value, (1, 0)))).astype(bf16)
    copies[3].wait()
    w_out = attn[3].astype(bf16)
    mixed = dot(attended, w_out, (1, 0)).astype(bf16)
    copies[8].wait()
    w_top = dense[:D].astype(bf16)
    w_low = dense[D:].astype(bf16)
    pre = dot(goals, w_top, (1, 0)) + dot(mixed, w_low, (1, 0)) + head[0:1, :]
    inner = 0.5 * (1.0 + lax.erf(pre * 0.5**0.5))
    hidden = (pre * inner).astype(bf16).astype(f32)
    head_vector = head[1:2, :].astype(bf16).astype(f32)
    logits = jnp.sum(hidden * head_vector, axis=1, keepdims=True)
    marks = column(labels)
    labeled = marks >= 0
    click = jnp.where(labeled, marks, 0).astype(f32)
    small = jnp.exp(-jnp.abs(logits))
    soft = jnp.maximum(logits, 0.0) + jnp.log1p(small)
    loss = jnp.sum(jnp.where(labeled, soft - click * logits, 0.0), axis=0, keepdims=True)
    count = jnp.sum(jnp.where(labeled, 1.0, 0.0), axis=0, keepdims=True)

    chance = jnp.where(logits >= 0, 1.0, small) / (1.0 + small)
    d_logits = jnp.where(labeled, chance - click, 0.0)
    d_hidden = (d_logits * head_vector).astype(bf16).astype(f32)
    d_pre = d_hidden * (inner + pre * jnp.exp(-0.5 * pre * pre) * (2.0 * jnp.pi) ** -0.5)
    d_pre_halves = halves(d_pre)
    d_mixed = both(dot(d_pre_halves, w_low, (1, 1))).astype(bf16)
    d_attended = dot(d_mixed, w_out, (1, 1)).astype(bf16)
    d_blocks = spread(d_attended.astype(f32))
    value_fold = dot(d_blocks.astype(bf16), w_value, (1, 1))
    d_attend = rows_by_user(value_fold, (1, 1)).astype(bf16).astype(f32)
    d_scores = weight * (d_attend - jnp.sum(weight * d_attend, axis=1, keepdims=True))
    d_scores = jnp.where(excluded, 0.0, d_scores)
    score_rows = rows_by_user(d_scores, (1, 0)) * DH ** (-0.5)
    d_queries = fold(both(dot(halves(score_rows), w_key, (1, 0)))).astype(bf16)

    def outer(a, b):
        return dot(a, b, (0, 0))

    def twice(x):
        return jnp.concatenate([x, x], axis=0)

    grads = [
        outer(goals, d_queries),
        outer(halves(score_rows), twice(query_blocks.astype(bf16))),
        outer(halves(mean_rows), twice(d_blocks.astype(bf16))),
        outer(attended, d_mixed),
    ]
    for i in range(4):
        for part in range(2):
            rows[pl.ds(512 * i + part, D, stride=2), :] = grads[i][:, LANES * part : LANES * (part + 1)]
    for source in range(2):
        grad = outer(twice((goals, mixed)[source]), d_pre_halves)
        for part in range(8):
            rows[pl.ds(2048 + 2048 * source + part, D, stride=8), :] = grad[:, LANES * part : LANES * (part + 1)]
    d_bias = jnp.sum(d_pre, axis=0, keepdims=True)
    d_vector = jnp.sum(d_logits * hidden, axis=0, keepdims=True)
    for source in range(2):
        grad = (d_bias, d_vector)[source]
        for part in range(8):
            at = 6144 + 8 * source + part
            rows[at : at + 1, :] = grad[:, LANES * part : LANES * (part + 1)]

    lane = iota((UNIT - 4 * MAIN - 4, LANES), 1)
    totals = jnp.where(lane == 0, loss, jnp.where(lane == 1, count, 0.0))

    def place(half, out):
        for main, tail, start, _ in windows(half):
            out[main : main + MAIN, :] = rows[start : start + MAIN, :]
            out[tail : tail + 1, :] = rows[start + MAIN : start + MAIN + 1, :]
        for unit in range(32):
            out[UNIT * unit + 4 * MAIN + 4 : UNIT * (unit + 1), :] = totals

    core = lax.axis_index("c")

    @pl.when(core == 0)
    def _():
        place(0, keep)
        place(1, send)

    @pl.when(core == 1)
    def _():
        place(1, keep)
        place(0, send)


VMEM = pl.BlockSpec(memory_space=pltpu.VMEM)
SMEM = pl.BlockSpec(memory_space=pltpu.SMEM)
HBM = pl.BlockSpec(memory_space=pltpu.HBM)


def vmem(*shape):
    return jax.ShapeDtypeStruct(shape, f32)


def call(body, outs, *args, specs=None, out_specs=None, scratch=(), limit=8):
    return pl.pallas_call(
        body,
        out_shape=outs,
        in_specs=specs or [VMEM] * len(args),
        out_specs=out_specs or jax.tree.map(lambda _: VMEM, outs),
        scratch_shapes=scratch,
        compiler_params=pltpu.CompilerParams(vmem_limit_bytes=limit * 2**20),
    )(*args)


def bit_here(part, step):
    x, y, c = (lax.axis_index(a) for a in ("x", "y", "c"))
    return jnp.where(
        c == 0, bit_of_traced(along(part, step), x, y), bit_of_traced(along(2 + part, step), x, y)
    )


def bit_of_traced(bit, x, y):
    v = x if bit < 2 else y
    q = v // 2
    return q if bit % 2 else (v + q) % 2


def first_split_body(keep, got, *outs):
    for part in range(2):
        half = STREAM // 2
        bit = bit_here(part, 0)
        for k in range(2):
            start = pl.multiple_of(STREAM * part + (bit if k == 0 else 1 - bit) * half, 8)
            outs[2 * part + k][...] = keep[pl.ds(start, half), :] + got[pl.ds(start, half), :]


def split_body(step):
    def body(own_0, got_0, own_1, got_1, *outs):
        for part, (own, got) in enumerate(((own_0, got_0), (own_1, got_1))):
            half = own.shape[0] // 2
            bit = bit_here(part, step)
            for k in range(2):
                start = pl.multiple_of((bit if k == 0 else 1 - bit) * half, 8)
                outs[2 * part + k][...] = own[pl.ds(start, half), :] + got[pl.ds(start, half), :]

    return body


def z_split_body(own_0, got_0, own_1, got_1, out):
    for part, (own, got) in enumerate(((own_0, got_0), (own_1, got_1))):
        total = own[...] + got[...]
        for k in range(4):
            out[4 * part + k, :MAIN, :] = total[MAIN * k : MAIN * (k + 1)]
            tail = total[4 * MAIN + k : 4 * MAIN + k + 1]
            at = iota((8, LANES), 0)
            out[4 * part + k, MAIN:, :] = jnp.where(at == 0, tail, jnp.where(at == 1, total[UNIT - 1 :], 0.0))


def adam_body(parts, moments, spread, new_moments, loss_out):
    total = parts[0]
    for z in range(1, 8):
        total = total + parts[z]
    zl, x, c = (lax.axis_index(a) for a in ("zl", "x", "c"))
    shift = 8 * (8 * zl + 2 * x + c)
    loss = total[MAIN + 1 : MAIN + 2, 0:1]
    count = total[MAIN + 1 : MAIN + 2, 1:2]
    loss_out[...] = loss / count
    lanes = iota((32, LANES), 1)
    turned = pltpu.roll(total, (LANES - shift) % LANES, 1)
    after = pltpu.roll(turned, 31, 0)
    grads = jnp.where(lanes < LANES - shift, turned, after) / count
    old = []
    for k in range(24):
        old.append(moments[:, LANES * k : LANES * (k + 1)])
    last = moments[:, SHARE - LANES :]
    last = jnp.where(iota((2, LANES), 1) < SHARE - 24 * LANES, pltpu.roll(last, SHARE - 24 * LANES, 1), 1.0)
    old.append(last)
    one = jnp.ones((7, LANES), f32)
    first = jnp.concatenate([o[0:1] for o in old] + [one], axis=0)
    second = jnp.concatenate([o[1:2] for o in old] + [one], axis=0)
    new_first = first_decay * first + (1.0 - first_decay) * grads
    new_second = second_decay * second + (1.0 - second_decay) * grads * grads
    for k in range(25):
        wide = min(LANES, SHARE - LANES * k)
        new_moments[0:1, LANES * k : LANES * k + wide] = new_first[k : k + 1, :wide]
        new_moments[1:2, LANES * k : LANES * k + wide] = new_second[k : k + 1, :wide]
    step = learn_rate * (new_first / first_fix) / (jnp.sqrt(new_second / second_fix) + adam_eps)
    flat = iota((32, LANES), 0) * LANES + lanes
    step = jnp.where(flat < SHARE, step, 0.0)
    turned = pltpu.roll(step, shift, 1)
    before = pltpu.roll(turned, 1, 0)
    step = jnp.where(lanes >= shift, turned, before)
    for z in range(8):
        spread[z] = step


def z_join_body(parts, *outs):
    for part in range(2):
        for k in range(4):
            outs[part][MAIN * k : MAIN * (k + 1), :] = parts[4 * part + k, :MAIN, :]
            outs[part][4 * MAIN + k : 4 * MAIN + k + 1, :] = parts[4 * part + k, MAIN : MAIN + 1, :]
        outs[part][4 * MAIN + 4 :, :] = jnp.zeros((UNIT - 4 * MAIN - 4, LANES), f32)


def join_body(step):
    def body(own_0, got_0, own_1, got_1, *outs):
        for part, (own, got) in enumerate(((own_0, got_0), (own_1, got_1))):
            half = own.shape[0]
            bit = bit_here(part, step)
            base, out = (STREAM * part, outs[0]) if step == 0 else (0, outs[part])
            for k, source in enumerate((own, got)):
                start = pl.multiple_of(base + (bit if k == 0 else 1 - bit) * half, 8)
                out[pl.ds(start, half), :] = source[...]

    return body


def apply_body(mine, other, attn, dense, head, new_attn, new_dense, new_head, rows):
    def place(half, source):
        for main, tail, start, where in windows(half):
            rows[start + 1 : start + MAIN, :] = source[main + 1 : main + MAIN, :]

    def joints(even, odd):
        firsts, lasts = {}, {}
        for half, source in ((0, even), (1, odd)):
            for main, tail, start, where in windows(half):
                firsts[start] = (source, main)
                lasts[start + MAIN] = (source, tail)
        for at in sorted(firsts | lasts):
            total = [r[m : m + 1, :] for r, m in (d[at] for d in (firsts, lasts) if at in d)]
            rows[at : at + 1, :] = sum(total[1:], total[0])

    core = lax.axis_index("c")
    for c in range(2):

        @pl.when(core == c)
        def _():
            place(c, mine)
            place(1 - c, other)
            joints(*((mine, other) if c == 0 else (other, mine)))

    for i in range(4):
        for part in range(2):
            lanes = slice(LANES * part, LANES * (part + 1))
            new_attn[i, :, lanes] = attn[i, :, lanes] - rows[pl.ds(512 * i + part, D, stride=2), :]
    for part in range(8):
        lanes = slice(LANES * part, LANES * (part + 1))
        new_dense[:, lanes] = dense[:, lanes] - rows[pl.ds(2048 + part, 2 * D, stride=8), :]
    for source in range(2):
        for part in range(8):
            lanes = slice(LANES * part, LANES * (part + 1))
            at = 6144 + 8 * source + part
            new_head[source : source + 1, lanes] = head[source : source + 1, lanes] - rows[at : at + 1, :]


def places():
    for zh in range(4):
        for y in range(4):
            for zl in range(2):
                for x in range(4):
                    for c in range(2):
                        yield zh, y, zl, x, c


def number(zh, y, zl, x, c):
    return (((zh * 4 + y) * 2 + zl) * 4 + x) * 2 + c


def flips(part, step):
    pairs = []
    for zh, y, zl, x, c in places():
        bit = along(2 * c + part, step)
        bits = [bit_of(b, x, y) for b in range(4)]
        bits[bit] ^= 1
        to_x, to_y = unbits(bits)
        pairs.append((number(zh, y, zl, x, c), number(zh, to_y, zl, to_x, c)))
    return pairs


def exchange(part, step, x):
    return lax.ppermute(x, AXES, flips(part, step))


def swap(x):
    return lax.ppermute(x, "c", [(0, 1), (1, 0)])


def gradient_windows(targets, behaviors, topk_index, target_ids, behavior_ids, target_codes, behavior_codes, labels, attn_weights, dense_weights, head_weights):
    return call(
        grad_body,
        (vmem(2 * STREAM, LANES), vmem(2 * STREAM, LANES)),
        *(
            pltpu.with_memory_space_constraint(x, pltpu.HBM)
            for x in (
                target_ids,
                target_codes,
                labels,
                targets,
                topk_index,
                behavior_ids,
                behavior_codes,
                head_weights,
                behaviors,
                attn_weights,
                dense_weights,
            )
        ),
        specs=[HBM] * 11,
        scratch=[
            pltpu.VMEM((ROWS, LANES), f32),
            pltpu.SMEM((U,), jnp.int32),
            pltpu.SMEM((U,), jnp.int32),
            pltpu.SMEM((U,), jnp.int32),
            pltpu.VMEM((U, D), bf16),
            pltpu.VMEM((U, K), jnp.int32),
            pltpu.VMEM((U, HIST), jnp.int32),
            pltpu.VMEM((U, HIST), jnp.int32),
            pltpu.VMEM((2, FF), f32),
            pltpu.VMEM((U, HIST, D), bf16),
            pltpu.VMEM((4, D, D), f32),
            pltpu.VMEM((2 * D, FF), f32),
            pltpu.SemaphoreType.DMA((17,)),
        ],
        limit=32,
    )


def per_device(
    targets,
    behaviors,
    topk_index,
    target_ids,
    behavior_ids,
    target_codes,
    behavior_codes,
    labels,
    attn_weights,
    dense_weights,
    head_weights,
    moments,
):
    keep, send = gradient_windows(
        targets, behaviors, topk_index, target_ids, behavior_ids, target_codes, behavior_codes, labels, attn_weights, dense_weights, head_weights
    )
    size = STREAM // 2
    own_0, sent_0, own_1, sent_1 = call(first_split_body, (vmem(size, LANES),) * 4, keep, swap(send))
    for step in range(4):
        got_0, got_1 = exchange(0, step, sent_0), exchange(1, step, sent_1)
        size //= 2
        if step < 3:
            own_0, sent_0, own_1, sent_1 = call(
                split_body(step + 1), (vmem(size, LANES),) * 4, own_0, got_0, own_1, got_1
            )
    parts = call(z_split_body, vmem(8, 32, LANES), own_0, got_0, own_1, got_1)
    parts = lax.all_to_all(parts, ("zh", "zl"), 0, 0, tiled=True)
    parts, new_moments, loss = call(
        adam_body, (vmem(8, 32, LANES), vmem(2, SHARE), vmem(1, 1)), parts, moments
    )
    parts = lax.all_to_all(parts, ("zh", "zl"), 0, 0, tiled=True)
    size = UNIT
    own_0, own_1 = call(z_join_body, (vmem(size, LANES),) * 2, parts)
    for step in range(3, -1, -1):
        got_0, got_1 = exchange(0, step, own_0), exchange(1, step, own_1)
        size *= 2
        outs = (vmem(size, LANES),) * 2 if step else (vmem(2 * size, LANES),)
        own_0, *own_1 = call(join_body(step), outs, own_0, got_0, own_1, got_1)
        own_1 = own_1[0] if step else None
    own = own_0
    new_attention, new_dense, new_head = call(
        apply_body,
        (vmem(4, D, D), vmem(2 * D, FF), vmem(2, FF)),
        own,
        swap(own),
        attn_weights,
        dense_weights,
        head_weights,
        scratch=[pltpu.VMEM((ROWS, LANES), f32)],
        limit=20,
    )
    return (new_attention, new_dense, new_head, new_moments, loss[0, 0])


def solution(mesh):
    finer = Mesh(mesh.devices.reshape(4, 4, 2, 4, 2), AXES)
    placed = (
        P(AXES, None),
        P(AXES, None, None),
        P(AXES, None),
        P(AXES),
        P(AXES, None),
        P(AXES),
        P(AXES, None),
        P(AXES),
        P(),
        P(),
        P(),
        P(None, AXES),
    )
    return jax.shard_map(
        per_device,
        mesh=finer,
        in_specs=placed,
        out_specs=(P(), P(), P(), P(None, AXES), P()),
        check_vma=False,
    )
```
